512 devices in a mesh: row: 128 (over x, z, core), col: 4 (over y).
Axes of the slice: x: 4, y: 4, z: 16, core: 2. Of those that a mesh axis runs over, the one named last changes fastest.
Arguments:
- right_sides: float32 [64, 6, 256, 128], P('col', None, 'row'), may hold values from -6 to 6
- inverse_diag: float32 [6, 256, 128, 128], P(None, 'row', 'col'), as said below
- off_blocks: bfloat16 [5, 256, 6, 128, 128], P(None, 'row', None, 'col'), may hold values from -0.109375 to 0.109375
- block_refs: int32 [5, 256, 6], P(None, 'row'), may hold values from 0 to 1279, as said below
Outputs:
- solution: float32 [64, 6, 256, 128], P('col', None, 'row')
The draws below stay inside these ranges and needn't reach their ends.
Inputs may be any that keep to these rules, and one draw needn't show every extreme that they name: block_refs[l, q, k] = lev * 256 + p names a block row of an earlier level, lev <= l. With p held by index p // 2 of row and the block rows q of level l held by index q // 2, the 12 entries of one device's rows at one level name at most 1 block rows held by any one device, and exactly 1 for some. `inverse_diag`: each block is the inverse of a nonsingular diagonal block of the factor.
All inputs are finite; a program needn't handle non-finite values.
Results may differ from the reference program's by a relative error of at most 0.0015.
Values may be sent and summed in bfloat16 or wider, within the bound.
A program may use at most 64 MiB of HBM per device.

```python
import jax
import jax.numpy as jnp
from jax import lax

BS = 128
NRHS = 64
LEVELS = 6
NOFF = 6
BPD = 2
LEVROWS = 256


def draw_inverse_diag(key, part):
    eye_block = jnp.eye(BS, dtype=jnp.float32)
    shape_diag = (LEVELS, LEVROWS, BS, 1)
    shape_full = (LEVELS, LEVROWS, BS, BS)
    diag_vals = jax.random.uniform(jax.random.fold_in(key, 21), shape_diag, jnp.float32, 0.7, 1.3)
    noise = jax.random.normal(jax.random.fold_in(key, 22), shape_full, jnp.float32) * (0.4 / BS ** 0.5)
    return eye_block * diag_vals + noise


def draw_block_refs(key, part):
    row_devs = LEVROWS // BPD
    count = (LEVELS - 1) * row_devs
    keys = jax.random.split(jax.random.fold_in(key, 11), count)
    perms = jax.vmap(lambda k: jax.random.permutation(k, row_devs))(keys)
    slot_ids = jnp.arange(BPD * NOFF, dtype=jnp.int32) % row_devs
    owners = perms[:, slot_ids].reshape(LEVELS - 1, LEVROWS, NOFF)
    shape = (LEVELS - 1, LEVROWS, NOFF)
    limits = (jnp.arange(LEVELS - 1, dtype=jnp.int32) + 1)[:, None, None] * jnp.ones((1, LEVROWS, NOFF), jnp.int32)
    source_level = jax.random.randint(jax.random.fold_in(key, 12), shape, 0, limits)
    which_row = jax.random.randint(jax.random.fold_in(key, 13), shape, 0, BPD)
    return (source_level * LEVROWS + owners * BPD + which_row).astype(jnp.int32)


def block_scale(rng, extent, cuts, low, high):
    def one(position, blocks):
        draws = jax.random.uniform(jax.random.fold_in(jax.random.fold_in(rng, 6), position), (blocks,), jnp.float32, low / len(cuts), high / len(cuts))
        return jnp.repeat(jnp.exp(draws), extent[position] // blocks).reshape((-1,) + (1,) * (len(extent) - position - 1))

    loudness = one(*cuts[0])
    for cut in cuts[1:]:
        loudness = loudness * one(*cut)
    return loudness


def centred(rng, shape, width, reach, shards=(), kind=jnp.bfloat16):
    factor_of = block_scale(rng, shape, shards, -0.22, 0.18) if shards else 1.0
    drawn = jax.random.normal(rng, shape, jnp.float32) * width * factor_of
    return jnp.minimum(jnp.maximum(drawn, -reach), reach).astype(kind)


def setup_inputs(seed: int = 0) -> dict:
    splits = jax.random.split(jax.random.key(seed), 5)
    right_sides = centred(splits[0], (NRHS, LEVELS, LEVROWS, BS), 1.0, 6.0, ((0, 4), (2, 128)), jnp.float32)
    inverse_diag = draw_inverse_diag(jax.random.fold_in(splits[4], 71), 0)
    off_blocks = centred(splits[2], (LEVELS - 1, LEVROWS, NOFF, BS, BS), (4 * NOFF * BS) ** -0.5, 0.109375, ((1, 128), (3, 4)))
    block_refs = draw_block_refs(jax.random.fold_in(splits[4], 71), 0)
    return {"right_sides": right_sides, "inverse_diag": inverse_diag, "off_blocks": off_blocks, "block_refs": block_refs}


def reference(right_sides, inverse_diag, off_blocks, block_refs):
    levels = right_sides.shape[1]
    history = []
    results = []
    for level_idx in range(levels):
        remainder = jnp.transpose(right_sides[:, level_idx], (1, 0, 2))
        if level_idx > 0:
            panel_table = jnp.concatenate(history, 0)
            fetched = panel_table[block_refs[level_idx - 1]]
            contrib = jnp.einsum("rkij,rkcj->rci", off_blocks[level_idx - 1].astype(jnp.float32),
                                 fetched.astype(jnp.float32), precision=lax.Precision.HIGHEST)
            remainder = remainder - contrib
        solved = jnp.einsum("rij,rcj->rci", inverse_diag[level_idx], remainder,
                            precision=lax.Precision.HIGHEST)
        results.append(solved)
        history.append(solved.astype(jnp.bfloat16))
    return jnp.transpose(jnp.stack(results, 0), (2, 0, 1, 3))
```

```python
import functools

import jax
import jax.numpy as jnp
from jax import lax
from jax.experimental import pallas as pl
from jax.experimental.pallas import tpu as pltpu
from jax.sharding import PartitionSpec as P

MESH = pl.DeviceIdType.MESH
NX, NZ, NY = 4, 16, 4
OWN = 3
GROUPS = (((1, 2, 3, -1, -2, -3), ((0, 7),)), ((4, 5, 6, -4, -5, -6), ((7, 3), (13, 3))), ((8, 7, -7), ((10, 3),)))


def kernel(refs, refs_hbm, b_ref, inv_hbm, off_hbm, out_ref, *scratch):
    (t0, t1, t2, t3, t4, offs, invs, bpart, xs, refs_v, refs_p,
     z_send, z_recv, x_send, x_recv, off_send, off_recv, off_own, inv_send, inv_recv, inv_own,
     b_send, b_recv, r_send, r_recv, r_own, out_send, out_recv) = scratch
    tables = (t0, t1, t2, t3, t4)
    levels = out_ref.shape[0]
    half = b_ref.shape[2] // 2
    rows = inv_hbm.shape[2]

    row = lax.axis_index("row")
    y = lax.axis_index("col")
    core = row % 2
    z = (row // 2) % NZ
    x = row // (2 * NZ)

    def chip(dx, dz, other=0):
        xx = (x + dx) % NX
        zz = (z + dz) % NZ
        cc = 1 - core if other else core
        return (xx * NZ + zz) * 2 + cc

    z_peers = [8, 7, -7, 6, -6, 5, -5, 4, -4, 3, -3, 2, -2, 1, -1]
    z_dev = {d: (chip(0, d), y) for d in z_peers}
    x_dev = {e: (chip(e, 0), y) for e in (1, 2, 3)}
    partner = (chip(0, 0, 1), y)
    y_dev = [(1, partner)]
    for dy in (2, 1, 3):
        yy = (y + dy) % NY
        y_dev += [(0, (chip(0, 0), yy)), (1, (chip(0, 0, 1), yy))]

    barrier = pltpu.get_barrier_semaphore()
    everyone = list(z_dev.values()) + list(x_dev.values()) + [d for _, d in y_dev]
    for dev in everyone:
        pl.semaphore_signal(barrier, inc=1, device_id=dev, device_id_type=MESH)
    pl.semaphore_wait(barrier, len(everyone))

    def push(src, dst, send, recv, dev):
        pltpu.make_async_remote_copy(
            src_ref=src, dst_ref=dst, send_sem=send, recv_sem=recv, device_id=dev, device_id_type=MESH
        ).start()

    def landed(ref, sem):
        pltpu.make_async_copy(ref, ref, sem).wait()

    mine = pl.ds(pl.multiple_of(y * rows, rows), rows)
    my_rhs = pl.ds(pl.multiple_of(core * half, half), half)
    other_rhs = pl.ds(pl.multiple_of((1 - core) * half, half), half)

    def give_inv(lev):
        for slot, dev in y_dev:
            push(inv_hbm.at[lev], invs.at[lev, slot, :, mine], inv_send.at[lev], inv_recv.at[lev], dev)
        pltpu.make_async_copy(inv_hbm.at[lev], invs.at[lev, 0, :, mine], inv_own.at[lev]).start()

    def give_off(lev):
        for slot, dev in y_dev:
            push(off_hbm.at[lev], offs.at[lev, slot, :, :, mine], off_send.at[lev], off_recv.at[lev], dev)
        pltpu.make_async_copy(off_hbm.at[lev], offs.at[lev, 0, :, :, mine], off_own.at[lev]).start()

    def seven(buf):
        return buf.at[:, :, pl.ds(0, 7 * buf.shape[2] // 8)]

    def off_seven(buf):
        return buf.at[:, :, :, pl.ds(0, 7 * buf.shape[3] // 8)]

    give_inv(0)
    push(b_ref.at[:, :, other_rhs], bpart, b_send, b_recv, partner)
    push(refs_hbm, refs_v, r_send, r_recv, partner)
    give_off(0)
    give_inv(1)

    landed(refs_v, r_recv)
    copy_refs = pltpu.make_async_copy(refs_v, refs_p, r_own)
    copy_refs.start()
    copy_refs.wait()
    landed(bpart, b_recv)

    iota = lax.broadcasted_iota(jnp.int32, (2 * half, 128), 0)
    masks = [jnp.where((iota // half) == h, 1.0, 0.0).astype(jnp.bfloat16) for h in (0, 1)]

    def fetch(lev, slot, b, k):
        ref = refs[lev - 1, b, k] if slot == 0 else refs_p[lev - 1, b, k]
        src_lev = ref // (4 * NX * NZ)
        q = ref % (4 * NX * NZ)
        h = q % 2
        pc = (q // 2) % 2
        s = ((q // 4) % NZ - z + OWN + NZ) % NZ
        rx = (q // (4 * NZ) - x + NX) % NX
        pair = pc + core - 2 * pc * core
        tile = tables[0][rx, s, pair]
        for other in range(1, lev):
            tile = lax.select(src_lev == other, tables[other][rx, s, pair], tile)
        return tile * lax.select(h == 1, masks[1], masks[0])

    def contribution(lev, slot, b):
        tiles = [fetch(lev, slot, b, k) for k in range(offs.shape[3])]
        blocks = [offs[lev - 1, slot, b, k] for k in range(offs.shape[3])]
        both = lax.dot_general(
            jnp.concatenate(tiles, 1), jnp.concatenate(blocks, 1), (((1,), (1,)), ((), ())),
            preferred_element_type=jnp.float32,
        )
        return both[:half] + both[half:]

    for lev in range(levels):
        if lev > 0:
            landed(off_seven(offs.at[lev - 1]), off_recv.at[lev - 1])
            pltpu.make_async_copy(off_hbm.at[lev - 1], offs.at[lev - 1, 0, :, :, mine], off_own.at[lev - 1]).wait()
        landed(seven(invs.at[lev]), inv_recv.at[lev])
        pltpu.make_async_copy(inv_hbm.at[lev], invs.at[lev, 0, :, mine], inv_own.at[lev]).wait()

        for slot in (0, 1):
            panel = []
            for b in (0, 1):
                right = b_ref[lev, b, my_rhs] if slot == 0 else bpart[lev, b]
                if lev > 0:
                    right = right - contribution(lev, slot, b)
                solved = lax.dot_general(
                    right, invs[lev, slot, b], (((1,), (1,)), ((), ())),
                    precision=lax.Precision.HIGHEST, preferred_element_type=jnp.float32,
                )
                panel.append(solved)
                if slot == 0:
                    out_ref[lev, b, my_rhs] = solved
                else:
                    xs[lev, b] = solved
            if lev + 1 < levels:
                tables[lev][0, OWN, slot] = jnp.concatenate(panel, 0).astype(jnp.bfloat16)

        if lev + 1 < levels:
            table = tables[lev]
            group_of = {d: g for g, (ds, _) in enumerate(GROUPS) for d in ds}
            for d in z_peers:
                push(table.at[0, OWN], table.at[0, (OWN - d) % NZ], z_send.at[lev], z_recv.at[lev, group_of[d]], z_dev[d])
            push(xs.at[lev], out_ref.at[lev, :, my_rhs], out_send, out_recv, partner)
            if lev + 2 < levels:
                give_off(lev + 1)
                give_inv(lev + 2)
            for g, (ds, spans) in enumerate(GROUPS):
                landed(table.at[0, pl.ds(0, len(ds))], z_recv.at[lev, g])
                for e in (2, 1, 3):
                    for at, size in spans:
                        push(table.at[0, pl.ds(at, size)], table.at[NX - e, pl.ds(at, size)],
                             x_send.at[lev], x_recv.at[lev], x_dev[e])
            landed(table.at[pl.ds(1, 3)], x_recv.at[lev])
        else:
            push(xs.at[lev], out_ref.at[lev, :, my_rhs], out_send, out_recv, partner)

    landed(bpart, b_send)
    landed(refs_v, r_send)
    for lev in range(levels):
        landed(seven(invs.at[lev]), inv_send.at[lev])
        if lev + 1 < levels:
            landed(off_seven(offs.at[lev]), off_send.at[lev])
            landed(tables[lev].at[0, pl.ds(0, 15)], z_send.at[lev])
            landed(tables[lev].at[pl.ds(1, 3)], x_send.at[lev])
    landed(xs, out_send)
    landed(xs, out_recv)


def shards(right_sides, inverse_diag, off_blocks, block_refs):
    rhs, levels, bpd, bs = right_sides.shape
    noff = off_blocks.shape[2]
    half = rhs // 2
    steps = levels - 1
    b = jnp.transpose(right_sides, (1, 2, 0, 3))
    dma = pltpu.SemaphoreType.DMA
    out = pl.pallas_call(
        kernel,
        out_shape=jax.ShapeDtypeStruct((levels, bpd, rhs, bs), jnp.float32),
        in_specs=[
            pl.BlockSpec(memory_space=pltpu.SMEM),
            pl.BlockSpec(memory_space=pl.ANY),
            pl.BlockSpec(memory_space=pltpu.VMEM),
            pl.BlockSpec(memory_space=pl.ANY),
            pl.BlockSpec(memory_space=pl.ANY),
        ],
        out_specs=pl.BlockSpec(memory_space=pltpu.VMEM),
        scratch_shapes=[pltpu.VMEM((NX, NZ, 2, 2 * half, bs), jnp.bfloat16)] * steps
        + [
            pltpu.VMEM((steps, 2, bpd, noff, bs, bs), jnp.bfloat16),
            pltpu.VMEM((levels, 2, bpd, bs, bs), jnp.float32),
            pltpu.VMEM((levels, bpd, half, bs), jnp.float32),
            pltpu.VMEM((levels, bpd, half, bs), jnp.float32),
            pltpu.VMEM(block_refs.shape, jnp.int32),
            pltpu.SMEM(block_refs.shape, jnp.int32),
            dma((steps,)), dma((steps, 3)), dma((steps,)), dma((steps,)),
            dma((steps,)), dma((steps,)), dma((steps,)),
            dma((levels,)), dma((levels,)), dma((levels,)),
            dma, dma, dma, dma, dma, dma, dma,
        ],
        compiler_params=pltpu.CompilerParams(collective_id=0, has_side_effects=True),
    )(block_refs, block_refs, b, inverse_diag, off_blocks)
    return jnp.transpose(out, (2, 0, 1, 3))


def solution(mesh):
    return jax.shard_map(
        shards,
        mesh=mesh,
        in_specs=(
            P("col", None, "row", None),
            P(None, "row", "col", None),
            P(None, "row", None, "col", None),
            P(None, "row", None),
        ),
        out_specs=P("col", None, "row", None),
        check_vma=False,
    )
```
